32 devices in a mesh: groups: 2 (over y), expert: 4 (over x, core), tensor: 4 (over z).
Axes of the slice: x: 2, y: 2, z: 4, core: 2. Of those that a mesh axis runs over, the one named last changes fastest.
Arguments:
- tokens: bfloat16 [512, 4096], P(('groups', 'expert'), 'tensor'), parts along dimension 0, may hold values from -400 to 400
- norm_gain: float32 [4096], replicated, may hold values from 0.5 to 1.5
- w_gate: bfloat16 [4096, 65536], P(None, ('expert', 'tensor')), may hold values from -0.09375 to 0.09375
- w_up: bfloat16 [4096, 65536], P(None, ('expert', 'tensor')), may hold values from -0.09375 to 0.09375
- w_down: bfloat16 [65536, 4096], P(('expert', 'tensor')), may hold values from -0.0625 to 0.0625
- expert_ids: int32 [512, 2], P(('groups', 'expert')), parts along dimension 0, may hold values from 0 to 7, all different within a row; in each aligned block of 64 rows (0 to 63, 64 to 127, ...) at most 32 rows name the same one
- gate_weights: float32 [512, 2], P(('groups', 'expert')), parts along dimension 0, may hold values from 0.1 to 1
Outputs:
- moe_out: bfloat16 [512, 4096], P(('groups', 'expert'), 'tensor'), parts along dimension 0
The draws below stay inside these ranges and needn't reach their ends.
There are 2 independent parts, one for each index of `groups`. The reference program is written for one: setup_inputs(seed, part) draws one part's arguments, and reference() takes and returns one part's arrays. A program takes and returns all parts, laid end to end along the dimension named above; an argument that names none is the same for every part. Nothing has to cross between parts.
Inputs may be any that keep to these rules, and one draw needn't show every extreme that they name: `expert_ids`: each request names two different experts. Within the rows of one device (aligned blocks of 64 rows) no expert is named by more than 32 rows, and in some blocks one expert is named by exactly 32 rows.
All inputs are finite; a program needn't handle non-finite values.
Results may differ from the reference program's by a relative error of at most 0.008.
Values may be sent and summed in bfloat16 or wider, within the bound.
A program may use at most 192 MiB of HBM per device.

```python
import math
import jax
import jax.numpy as jnp
import numpy as np
from jax import lax

WIDTH = 4096
EXPERT_HIDDEN = 8192
EXPERTS = 8
TOK_DEV = 64
SLOTS = 32
TOKENS = 256
N_EXPERT = 4


def draw_tokens(key, part):
    key_base, key_rows, key_cols = jax.random.split(key, 3)
    row_scale = jnp.exp(jax.random.uniform(key_rows, (TOKENS, 1), jnp.float32, 0.0, 2.3))
    ramp = jnp.exp(jnp.log(3.0) * jnp.arange(WIDTH, dtype=jnp.float32) / WIDTH)
    col_scale = ramp[None, :] * jnp.exp(jax.random.uniform(key_cols, (1, WIDTH), jnp.float32, -1.15, 1.15))
    base = jax.random.truncated_normal(key_base, -4.0, 4.0, (TOKENS, WIDTH), jnp.float32)
    return jnp.clip(base * row_scale * col_scale, -400.0, 400.0).astype(jnp.bfloat16)


def level_of(own_key, shape, shards, least, largest):
    gain, own = 1.0, jax.random.fold_in(own_key, 6)
    for dim, blocks in shards:
        draws = jnp.exp(jax.random.uniform(jax.random.fold_in(own, dim), (blocks,), jnp.float32, least / len(shards), largest / len(shards)))
        gain = gain * jnp.repeat(draws, shape[dim] // blocks).reshape([-1 if axis == dim else 1 for axis in range(len(shape))])
    return gain


def shared_out(stream_key, own, number, rows, amount, top, most, skew):
    sequence = jax.random.permutation(stream_key, amount)
    packed, usual = shares(amount, rows * top, most, skew, True), shares(amount, rows * top, most, skew, False)
    places = jnp.arange(amount)

    def named(sizes, turn):
        used = int((sizes > 0).sum())
        fixed = max(1, used // 4)
        shifted = fixed + (places - fixed + turn * (used - fixed)) % max(1, amount - fixed)
        return jnp.zeros((amount,), jnp.int32).at[sequence[jnp.where(places < fixed, places, shifted)]].set(jnp.asarray(sizes, jnp.int32))

    sizes = jnp.where(number % 4 == 0, named(packed, number // 4), named(usual, number - number // 4 - 1))
    mixed = jax.random.permutation(jax.random.fold_in(own, 3), amount)
    donor, receiver = mixed[0:amount // 2 * 2:2], mixed[1:amount // 2 * 2:2]
    room = jnp.minimum(sizes[donor] - 1, most - sizes[receiver]) // 2
    room = jnp.where((donor == sequence[0]) | (receiver == sequence[0]) | (sizes[receiver] == 0), 0, jnp.maximum(room, 0))
    shifted = jax.random.randint(jax.random.fold_in(own, 4), (amount // 2,), 0, 1 << 20) % (room + 1)
    sizes = sizes.at[donor].add(-shifted).at[receiver].add(shifted)
    members = jnp.searchsorted(jnp.cumsum(sizes), jnp.arange(rows * top), side="right").astype(jnp.int32)
    grid = members.reshape(top, rows).T
    grid = grid[jax.random.permutation(jax.random.fold_in(own, 1), rows)]
    turn = jax.random.randint(jax.random.fold_in(own, 2), (rows, 1), 0, top)
    return jnp.take_along_axis(grid, (jnp.arange(top)[None, :] + turn) % top, axis=1)


def shares(number_of, total, most, skew, full):
    weights = [(1 << 20) // math.isqrt(rank ** skew) + 1 for rank in range(1, number_of + 1)]
    largest = most if full else min(most, max(-(-total // number_of), total * weights[0] // sum(weights)))
    least = 1 if total - largest >= number_of - 1 else 0
    given, surplus = [largest] + [least] * (number_of - 1), total - largest - least * (number_of - 1)
    while surplus > 0:
        free = [i for i in range(1, number_of) if given[i] < largest] or [i for i in range(1, number_of) if given[i] < most]
        whole, remaining = sum([weights[i] for i in free]), surplus
        for i in free:
            more = min(most - given[i], max(1, remaining * weights[i] // whole), surplus)
            given[i] = given[i] + more
            surplus = surplus - more
    return np.array(given)


def scatter_about(stream_key, extent, deviation, reach, cuts=(), held_as=jnp.bfloat16):
    level = level_of(stream_key, extent, cuts, -0.22, 0.18) if cuts else 1.0
    values = jax.random.normal(stream_key, extent, jnp.float32) * deviation * level
    return jnp.minimum(jnp.maximum(values, -reach), reach).astype(held_as)


def setup_inputs(seed: int = 0, part: int = 0) -> dict:
    splits = jax.random.split(jax.random.key(seed), 8)
    part_splits = jax.random.split(jax.random.fold_in(splits[7], part), 8)
    tokens = draw_tokens(jax.random.fold_in(jax.random.fold_in(splits[7], part), 71), part)
    norm_gain = jnp.clip(1.0 + 0.1 * jax.random.normal(splits[1], (WIDTH,), jnp.float32), 0.5, 1.5)
    w_gate = scatter_about(splits[2], (WIDTH, EXPERTS * EXPERT_HIDDEN), WIDTH ** -0.5, 0.09375, ((1, 16),))
    w_up = scatter_about(splits[3], (WIDTH, EXPERTS * EXPERT_HIDDEN), WIDTH ** -0.5, 0.09375, ((1, 16),))
    w_down = scatter_about(splits[4], (EXPERTS * EXPERT_HIDDEN, WIDTH), EXPERT_HIDDEN ** -0.5, 0.0625, ((0, 16),))
    expert_ids_keys = jax.random.split(jax.random.fold_in(part_splits[5], 1), TOKENS // TOK_DEV)
    expert_ids_turns = jax.random.permutation(jax.random.fold_in(part_splits[5], 3), TOKENS // TOK_DEV)
    expert_ids = jax.vmap(lambda own, number: shared_out(jax.random.fold_in(part_splits[5], 2), own, number, TOK_DEV, EXPERTS, 2, SLOTS, 2))(expert_ids_keys, expert_ids_turns).reshape((TOKENS, 2))
    gate_weights = jnp.clip(0.1 + 0.9 * jax.random.uniform(part_splits[6], (TOKENS, 2), jnp.float32) ** level_of(part_splits[6], (TOKENS, 2), ((0, 4),), -0.2, 0.2), 0.1, 1.0)
    return {"tokens": tokens, "norm_gain": norm_gain, "w_gate": w_gate, "w_up": w_up, "w_down": w_down, "expert_ids": expert_ids, "gate_weights": gate_weights}


def reference(tokens, norm_gain, w_gate, w_up, w_down, expert_ids, gate_weights):
    values = tokens.astype(jnp.float32)
    mean_square = lax.optimization_barrier(jnp.mean(values * values, axis=1, keepdims=True))
    normed = (values * lax.rsqrt(mean_square + 1e-05) * norm_gain[None, :]).astype(jnp.bfloat16)
    capacity_all = N_EXPERT * SLOTS
    result = jnp.zeros((TOKENS, WIDTH), jnp.float32)
    for expert in range(EXPERTS):
        chosen = expert_ids == expert
        weight_of = lax.optimization_barrier(jnp.sum(jnp.where(chosen, gate_weights, jnp.zeros_like(gate_weights)), axis=1))
        is_routed = jnp.any(chosen, axis=1).astype(jnp.int32)
        picked = jnp.argsort(1 - is_routed, stable=True)[:capacity_all].astype(jnp.int32)
        row_data = jnp.take(normed, picked, axis=0)
        low = expert * EXPERT_HIDDEN
        high = low + EXPERT_HIDDEN
        gate_act = jnp.dot(row_data, w_gate[:, low:high], preferred_element_type=jnp.float32)
        up_act = jnp.dot(row_data, w_up[:, low:high], preferred_element_type=jnp.float32)
        hidden = (jax.nn.silu(gate_act) * up_act).astype(jnp.bfloat16)
        expert_out = jnp.dot(hidden, w_down[low:high, :], preferred_element_type=jnp.float32)
        weights_here = jnp.take(weight_of, picked, axis=0)
        result = result.at[picked].add(weights_here[:, None] * expert_out)
    return result.astype(jnp.bfloat16)
```

```python
import functools

import jax
import jax.numpy as jnp
from jax import lax
from jax.experimental import pallas as pl
from jax.experimental.pallas import tpu as pltpu
from jax.sharding import PartitionSpec as P

EXPERTS = 8
MIB = 1 << 20
MESH = pl.DeviceIdType.MESH


def log2(value):
    power = value.bit_length() - 1
    assert 1 << power == value
    return power


def kernel(
    n_e, n_t, cap, chunk, pair_slots, lag,
    tokens, gain, meta, ids, w_gate, w_up, w_down,
    out,
    wbuf, blocks, metas, packed, hidden, wslot, place, sendbuf, recvbuf, zsend, zrecv,
    wsem, lsem, rsem, zsem, xsem, dsem, msend, mrecv, osend, orecv, ysend, yrecv,
):
    g, e, t = lax.axis_index("groups"), lax.axis_index("expert"), lax.axis_index("tensor")
    n_x = n_e // 2
    xi, core = e // 2, e % 2
    sibling = xi * 2 + (1 - core)
    rows, width_local = tokens.shape
    width = w_gate.shape[0]
    hid = w_gate.shape[1]
    per_expert = n_e * n_t // EXPERTS
    mine = (e * n_t + t) // per_expert
    gate_pairs = hid // chunk
    per_slice = width_local // chunk
    down_chunks = n_t * per_slice
    pairs = gate_pairs + down_chunks // 2

    def slice_of(s):
        return lax.rem(t + 1 + s, n_t)

    def weight_copy(src, slot):
        return pltpu.make_async_copy(src, wbuf.at[slot, pl.ds(0, src.shape[0])], wsem.at[slot])

    def columns(start, size):
        return pl.ds(pl.multiple_of(start, size), size)

    def down_columns(d):
        return columns(slice_of(d // per_slice) * width_local + (d % per_slice) * chunk, chunk)

    def start_pair(p):
        slot = (p % pair_slots) * 2

        @pl.when(p < gate_pairs)
        def _():
            cols = columns(p * chunk, chunk)
            weight_copy(w_gate.at[:, cols], slot).start()
            weight_copy(w_up.at[:, cols], slot + 1).start()

        @pl.when(jnp.logical_and(p >= gate_pairs, p < pairs))
        def _():
            d = (p - gate_pairs) * 2
            weight_copy(w_down.at[:, down_columns(d)], slot).start()
            weight_copy(w_down.at[:, down_columns(d + 1)], slot + 1).start()

    def block_copy(ej, q, send_sem, to):
        return pltpu.make_async_remote_copy(
            src_ref=blocks.at[ej, q], dst_ref=blocks.at[ej, q],
            send_sem=send_sem, recv_sem=rsem.at[ej, q], device_id=to, device_id_type=MESH,
        )

    def z_copy(s):
        return block_copy(e, t, zsem.at[s], (g, e, lax.rem(t + s, n_t)))

    def x_copy(o, s):
        return block_copy(e, lax.rem(t + s, n_t), xsem.at[o, s], (g, lax.rem(xi + o, n_x) * 2 + core, t))

    def d_copy(o, s):
        ej = lax.rem(xi + o, n_x) * 2 + core
        return block_copy(ej, lax.rem(t + s, n_t), dsem.at[o, s], (g, sibling, t))

    def arrived(ej, s):
        block_copy(ej, lax.rem(t + s, n_t), zsem.at[0], (g, sibling, t)).wait_recv()

    def meta_copy(o):
        return pltpu.make_async_remote_copy(
            src_ref=meta, dst_ref=metas.at[e], send_sem=msend.at[o], recv_sem=mrecv.at[e],
            device_id=(g, lax.rem(e + o, n_e), t), device_id_type=MESH,
        )

    def meta_arrived(o):
        ej = lax.rem(e + o, n_e)
        pltpu.make_async_remote_copy(
            src_ref=meta, dst_ref=metas.at[ej], send_sem=msend.at[0], recv_sem=mrecv.at[ej],
            device_id=(g, ej, t), device_id_type=MESH,
        ).wait_recv()

    own = pltpu.make_async_copy(tokens, blocks.at[e, t], lsem.at[0])
    own.start()
    own_meta = pltpu.make_async_copy(meta, metas.at[e], lsem.at[1])
    own_meta.start()
    barrier = pltpu.get_barrier_semaphore()
    for o in range(1, n_e):
        pl.semaphore_signal(barrier, inc=1, device_id=(g, lax.rem(e + o, n_e), t), device_id_type=MESH)
    for o in range(1, n_t):
        pl.semaphore_signal(barrier, inc=1, device_id=(g, e, lax.rem(t + o, n_t)), device_id_type=MESH)
    for p in range(min(pair_slots, pairs)):
        start_pair(jnp.int32(p))
    own.wait()
    own_meta.wait()

    slots = n_e * cap
    column = lax.broadcasted_iota(jnp.int32, (rows, slots), 1)
    expert_at = ((column >> log2(cap)) * n_t + t) >> log2(per_expert)
    member = jnp.logical_or(ids[:, 0:1] == expert_at, ids[:, 1:2] == expert_at)
    before = lax.broadcasted_iota(jnp.int32, (rows, rows), 1) < lax.broadcasted_iota(jnp.int32, (rows, rows), 0)
    rank = jnp.dot(
        before.astype(jnp.float32).astype(jnp.bfloat16),
        member.astype(jnp.float32).astype(jnp.bfloat16),
        preferred_element_type=jnp.float32,
    )
    hit = jnp.logical_and(member, rank == (column & (cap - 1)).astype(jnp.float32))
    place[...] = hit.astype(jnp.float32).astype(jnp.bfloat16)

    pl.semaphore_wait(barrier, n_e - 1 + n_t - 1)

    for o in range(1, n_e):
        meta_copy(o).start()
    for s in range(1, n_t):
        z_copy(s).start()

    lanes = meta.shape[1]
    upper = (
        lax.broadcasted_iota(jnp.int32, (lanes, lanes), 0) < lax.broadcasted_iota(jnp.int32, (lanes, lanes), 1)
    ).astype(jnp.float32).astype(jnp.bfloat16)

    def pick(ej):
        id0, id1 = metas[ej, 0:1, :], metas[ej, 1:2, :]
        target = mine.astype(jnp.float32)
        named = jnp.where(id0 == target, 1.0, 0.0) + jnp.where(id1 == target, 1.0, 0.0)
        order = jnp.dot(
            jnp.broadcast_to(named, (8, lanes)).astype(jnp.bfloat16), upper, preferred_element_type=jnp.float32
        )[0:1, :]
        slot = lax.broadcasted_iota(jnp.int32, (cap, lanes), 0).astype(jnp.float32)
        return jnp.where(slot == order, 1.0, 0.0) * named

    def pack(s):
        q = lax.rem(t + s, n_t)

        def one(ej, _):
            @pl.when(ej % 2 != core)
            def _():
                arrived(ej, s)

            select = pick(ej)[:, :rows].astype(jnp.bfloat16)
            picked = jnp.dot(select, blocks[ej, q], preferred_element_type=jnp.float32)
            packed[columns(ej * cap, cap), columns(q * width_local, width_local)] = picked.astype(jnp.bfloat16)
            return 0

        lax.fori_loop(0, n_e, one, 0)

    def relay(s):
        for o in range(1, n_x):
            arrived(lax.rem(xi + o, n_x) * 2 + core, s)
            d_copy(o, s).start()

    def forward(s):
        for o in range(1, n_x):
            x_copy(o, s).start()
        d_copy(0, s).start()

    forward(0)
    for o in range(1, n_e):
        meta_arrived(o)

    def dispatch(s, _):
        arrived(e, s)
        forward(s)
        relay(s - 1)
        pack(s - 1)
        return 0

    lax.fori_loop(1, n_t, dispatch, 0)
    relay(n_t - 1)
    pack(n_t - 1)

    def normalize(ej, _):
        at = columns(ej * cap, cap)
        weight = jnp.where(metas[ej, 0:1, :] == mine.astype(jnp.float32), metas[ej, 2:3, :], metas[ej, 3:4, :])
        wslot[at, :] = jnp.broadcast_to(jnp.sum(pick(ej) * weight, axis=1, keepdims=True), (cap, lanes))
        values = packed[at, :].astype(jnp.float32)
        scale = lax.rsqrt(jnp.sum(values * values, axis=1, keepdims=True) / width + 1e-05)
        packed[at, :] = (values * scale * gain[...]).astype(jnp.bfloat16)
        return 0

    lax.fori_loop(0, n_e, normalize, 0)

    def expert_in(j, _):
        slot = (j % pair_slots) * 2
        cols = columns(j * chunk, chunk)
        weight_copy(w_gate.at[:, cols], slot).wait()
        gate = jnp.dot(packed[...], wbuf[slot], preferred_element_type=jnp.float32)
        weight_copy(w_up.at[:, cols], slot + 1).wait()
        up = jnp.dot(packed[...], wbuf[slot + 1], preferred_element_type=jnp.float32)
        hidden[:, cols] = (gate / (1.0 + jnp.exp(-gate)) * up).astype(jnp.bfloat16)
        start_pair(j + pair_slots)
        return 0

    lax.fori_loop(0, gate_pairs, expert_in, 0)

    def o_copy(o, d):
        ej = lax.rem(e + o, n_e)
        return pltpu.make_async_remote_copy(
            src_ref=sendbuf.at[d, columns(ej * cap, cap)], dst_ref=recvbuf.at[d, columns(e * cap, cap)],
            send_sem=osend.at[o, d], recv_sem=orecv.at[e, d], device_id=(g, ej, t), device_id_type=MESH,
        )

    def o_arrived(o, d):
        ej = lax.rem(e + o, n_e)
        pltpu.make_async_remote_copy(
            src_ref=sendbuf.at[d, columns(ej * cap, cap)], dst_ref=recvbuf.at[d, columns(ej * cap, cap)],
            send_sem=osend.at[0, 0], recv_sem=orecv.at[ej, d], device_id=(g, ej, t), device_id_type=MESH,
        ).wait_recv()

    def y_copy(d):
        k, c = d // per_slice, d % per_slice
        return pltpu.make_async_remote_copy(
            src_ref=zsend.at[d], dst_ref=zrecv.at[t, c],
            send_sem=ysend.at[d], recv_sem=yrecv.at[t, c],
            device_id=(g, e, slice_of(k)), device_id_type=MESH,
        )

    def y_arrived(s, c):
        tj = lax.rem(t + s, n_t)
        pltpu.make_async_remote_copy(
            src_ref=zsend.at[0], dst_ref=zrecv.at[tj, c],
            send_sem=ysend.at[0], recv_sem=yrecv.at[tj, c],
            device_id=(g, e, tj), device_id_type=MESH,
        ).wait_recv()
        return zrecv[tj, c].astype(jnp.float32)

    def combined(d):
        for o in range(1, n_e):
            o_arrived(o, d)
        return jnp.dot(place[...], recvbuf[d], preferred_element_type=jnp.float32)

    def combine_and_send(d):
        zsend[d] = combined(d).astype(jnp.bfloat16)
        y_copy(d).start()

    def expert_out(d, _):
        slot = ((gate_pairs + d // 2) % pair_slots) * 2 + d % 2
        weight_copy(w_down.at[:, down_columns(d)], slot).wait()
        value = jnp.dot(hidden[...], wbuf[slot, 0:hid, :], preferred_element_type=jnp.float32)
        sendbuf[d] = (value * wslot[:, 0:1]).astype(jnp.bfloat16)
        for o in range(1, n_e):
            o_copy(o, d).start()
        at = columns(e * cap, cap)
        recvbuf[d, at, :] = sendbuf[d, at, :]

        @pl.when(d % 2 == 1)
        def _():
            start_pair(gate_pairs + d // 2 + pair_slots)

        @pl.when(jnp.logical_and(d >= lag, d - lag < down_chunks - per_slice))
        def _():
            combine_and_send(d - lag)

        return 0

    lax.fori_loop(0, down_chunks, expert_out, 0)

    def late(d, _):
        combine_and_send(d)
        return 0

    lax.fori_loop(max(0, down_chunks - lag), down_chunks - per_slice, late, 0)
    for c in range(per_slice):
        total = combined(down_chunks - per_slice + c)
        for s in range(1, n_t):
            total += y_arrived(s, c)
        out[:, c * chunk:(c + 1) * chunk] = total.astype(jnp.bfloat16)

    for o in range(1, n_e):
        meta_copy(o).wait_send()
    for s in range(1, n_t):
        z_copy(s).wait_send()

    def drain_blocks(s, _):
        for o in range(n_x):
            if o:
                x_copy(o, s).wait_send()
            d_copy(o, s).wait_send()
        return 0

    lax.fori_loop(0, n_t, drain_blocks, 0)

    def drain_rows(d, _):
        for o in range(1, n_e):
            o_copy(o, d).wait_send()
        return 0

    lax.fori_loop(0, down_chunks, drain_rows, 0)

    def drain_sums(d, _):
        y_copy(d).wait_send()
        return 0

    lax.fori_loop(0, down_chunks - per_slice, drain_sums, 0)


def per_device(n_e, n_t, tokens, norm_gain, w_gate, w_up, w_down, expert_ids, gate_weights):
    rows, width_local = tokens.shape
    width, hid = w_gate.shape
    cap = rows // 2
    slots = n_e * cap
    chunk = min(512, width_local, hid)
    per_slice = width_local // chunk
    down_chunks = n_t * per_slice
    pairs = hid // chunk + down_chunks // 2
    spent = 2 * (width * rows * n_e + slots * width + slots * hid + 2 * slots * width + 2 * rows * width)
    pair_slots = min(pairs, (56 * MIB - spent) // (4 * width * chunk))
    lanes = -(-rows // 128) * 128
    pad = lanes - rows
    meta = jnp.concatenate(
        [
            jnp.pad(expert_ids.T.astype(jnp.float32), ((0, 0), (0, pad)), constant_values=-1.0),
            jnp.pad(gate_weights.T, ((0, 4), (0, pad))),
        ],
        axis=0,
    )
    vmem = pl.BlockSpec(memory_space=pltpu.VMEM)
    hbm = pl.BlockSpec(memory_space=pl.ANY)
    bf16, f32, dma = jnp.bfloat16, jnp.float32, pltpu.SemaphoreType.DMA
    return pl.pallas_call(
        functools.partial(kernel, n_e, n_t, cap, chunk, pair_slots, 3),
        out_shape=jax.ShapeDtypeStruct((rows, width_local), bf16),
        in_specs=[vmem, vmem, vmem, vmem, hbm, hbm, hbm],
        out_specs=vmem,
        scratch_shapes=[
            pltpu.VMEM((2 * pair_slots, width, chunk), bf16),
            pltpu.VMEM((n_e, n_t, rows, width_local), bf16),
            pltpu.VMEM((n_e, 8, lanes), f32),
            pltpu.VMEM((slots, width), bf16),
            pltpu.VMEM((slots, hid), bf16),
            pltpu.VMEM((slots, lanes), f32),
            pltpu.VMEM((rows, slots), bf16),
            pltpu.VMEM((down_chunks, slots, chunk), bf16),
            pltpu.VMEM((down_chunks, slots, chunk), bf16),
            pltpu.VMEM((down_chunks, rows, chunk), bf16),
            pltpu.VMEM((n_t, per_slice, rows, chunk), bf16),
            dma((2 * pair_slots,)),
            dma((2,)),
            dma((n_e, n_t)),
            dma((n_t,)),
            dma((n_e // 2, n_t)),
            dma((n_e // 2, n_t)),
            dma((n_e,)),
            dma((n_e,)),
            dma((n_e, down_chunks)),
            dma((n_e, down_chunks)),
            dma((down_chunks,)),
            dma((n_t, per_slice)),
        ],
        compiler_params=pltpu.CompilerParams(
            collective_id=0, has_side_effects=True, vmem_limit_bytes=67043328
        ),
    )(tokens, norm_gain.reshape(1, width), meta, expert_ids, w_gate, w_up, w_down)


def solution(mesh):
    in_specs = (
        P(("groups", "expert"), "tensor"),
        P(),
        P(None, ("expert", "tensor")),
        P(None, ("expert", "tensor")),
        P(("expert", "tensor"), None),
        P(("groups", "expert"), None),
        P(("groups", "expert"), None),
    )
    out_specs = P(("groups", "expert"), "tensor")
    body = functools.partial(per_device, mesh.shape["expert"], mesh.shape["tensor"])
    return jax.shard_map(body, mesh=mesh, in_specs=in_specs, out_specs=out_specs, check_vma=False)
```

```python
import functools

import jax
import jax.numpy as jnp
from jax import lax
from jax.experimental import pallas as pl
from jax.experimental.pallas import tpu as pltpu
from jax.sharding import PartitionSpec as P

EXPERTS = 8
MIB = 1 << 20
MESH = pl.DeviceIdType.MESH


def log2(value):
    power = value.bit_length() - 1
    assert 1 << power == value
    return power


def kernel(
    n_e, n_t, cap, chunk, pair_slots, lag,
    tokens, gain, meta, ids, w_gate, w_up, w_down,
    out,
    wbuf, blocks, metas, packed, hidden, wslot, place, sendbuf, recvbuf, zsend, zrecv,
    wsem, lsem, rsem, zsem, xsem, dsem, msend, mrecv, osend, orecv, ysend, yrecv,
):
    g, e, t = lax.axis_index("groups"), lax.axis_index("expert"), lax.axis_index("tensor")
    n_x = n_e // 2
    xi, core = e // 2, e % 2
    sibling = xi * 2 + (1 - core)
    rows, width_local = tokens.shape
    width = w_gate.shape[0]
    hid = w_gate.shape[1]
    per_expert = n_e * n_t // EXPERTS
    mine = (e * n_t + t) // per_expert
    gate_pairs = hid // chunk
    per_slice = width_local // chunk
    down_chunks = n_t * per_slice
    pairs = gate_pairs + down_chunks // 2

    def slice_of(s):
        return lax.rem(t + 1 + s, n_t)

    def weight_copy(src, slot):
        return pltpu.make_async_copy(src, wbuf.at[slot, pl.ds(0, src.shape[0])], wsem.at[slot])

    def columns(start, size):
        return pl.ds(pl.multiple_of(start, size), size)

    def down_columns(d):
        return columns(slice_of(d // per_slice) * width_local + (d % per_slice) * chunk, chunk)

    def start_pair(p):
        slot = (p % pair_slots) * 2

        @pl.when(p < gate_pairs)
        def _():
            cols = columns(p * chunk, chunk)
            weight_copy(w_gate.at[:, cols], slot).start()
            weight_copy(w_up.at[:, cols], slot + 1).start()

        @pl.when(jnp.logical_and(p >= gate_pairs, p < pairs))
        def _():
            d = (p - gate_pairs) * 2
            weight_copy(w_down.at[:, down_columns(d)], slot).start()
            weight_copy(w_down.at[:, down_columns(d + 1)], slot + 1).start()

    def block_copy(ej, q, send_sem, to):
        return pltpu.make_async_remote_copy(
            src_ref=blocks.at[ej, q], dst_ref=blocks.at[ej, q],
            send_sem=send_sem, recv_sem=rsem.at[ej, q], device_id=to, device_id_type=MESH,
        )

    def z_copy(side, q):
        return block_copy(e, q, zsem.at[side, q], (g, e, lax.rem(t + 1 - 2 * side + n_t, n_t)))

    def x_copy(o, q):
        return block_copy(e, q, xsem.at[o, q], (g, lax.rem(xi + o, n_x) * 2 + core, t))

    def d_copy(o, q):
        ej = lax.rem(xi + o, n_x) * 2 + core
        return block_copy(ej, q, dsem.at[o, q], (g, sibling, t))

    def arrived(ej, q):
        block_copy(ej, q, zsem.at[0, 0], (g, sibling, t)).wait_recv()

    def has_next(side):
        return t < n_t - 1 if side == 0 else t > 0

    def at_distance(h, step):
        for side in (0, 1):
            q = t - h if side == 0 else t + h

            @pl.when(q >= 0 if side == 0 else q < n_t)
            def _():
                step(side, q)

    def meta_copy(o):
        return pltpu.make_async_remote_copy(
            src_ref=meta, dst_ref=metas.at[e], send_sem=msend.at[o], recv_sem=mrecv.at[e],
            device_id=(g, lax.rem(e + o, n_e), t), device_id_type=MESH,
        )

    def meta_arrived(o):
        ej = lax.rem(e + o, n_e)
        pltpu.make_async_remote_copy(
            src_ref=meta, dst_ref=metas.at[ej], send_sem=msend.at[0], recv_sem=mrecv.at[ej],
            device_id=(g, ej, t), device_id_type=MESH,
        ).wait_recv()

    own = pltpu.make_async_copy(tokens, blocks.at[e, t], lsem.at[0])
    own.start()
    own_meta = pltpu.make_async_copy(meta, metas.at[e], lsem.at[1])
    own_meta.start()
    barrier = pltpu.get_barrier_semaphore()
    for o in range(1, n_e):
        pl.semaphore_signal(barrier, inc=1, device_id=(g, lax.rem(e + o, n_e), t), device_id_type=MESH)
    for o in range(1, n_t):
        pl.semaphore_signal(barrier, inc=1, device_id=(g, e, lax.rem(t + o, n_t)), device_id_type=MESH)
    for p in range(min(pair_slots, pairs)):
        start_pair(jnp.int32(p))
    own.wait()
    own_meta.wait()

    slots = n_e * cap
    column = lax.broadcasted_iota(jnp.int32, (rows, slots), 1)
    expert_at = ((column >> log2(cap)) * n_t + t) >> log2(per_expert)
    member = jnp.logical_or(ids[:, 0:1] == expert_at, ids[:, 1:2] == expert_at)
    before = lax.broadcasted_iota(jnp.int32, (rows, rows), 1) < lax.broadcasted_iota(jnp.int32, (rows, rows), 0)
    rank = jnp.dot(
        before.astype(jnp.float32).astype(jnp.bfloat16),
        member.astype(jnp.float32).astype(jnp.bfloat16),
        preferred_element_type=jnp.float32,
    )
    hit = jnp.logical_and(member, rank == (column & (cap - 1)).astype(jnp.float32))
    place[...] = hit.astype(jnp.float32).astype(jnp.bfloat16)

    pl.semaphore_wait(barrier, n_e - 1 + n_t - 1)

    for o in range(1, n_e):
        meta_copy(o).start()
    for side in (0, 1):
        @pl.when(has_next(side))
        def _():
            z_copy(side, t).start()

    lanes = meta.shape[1]
    upper = (
        lax.broadcasted_iota(jnp.int32, (lanes, lanes), 0) < lax.broadcasted_iota(jnp.int32, (lanes, lanes), 1)
    ).astype(jnp.float32).astype(jnp.bfloat16)

    def pick(ej):
        id0, id1 = metas[ej, 0:1, :], metas[ej, 1:2, :]
        target = mine.astype(jnp.float32)
        named = jnp.where(id0 == target, 1.0, 0.0) + jnp.where(id1 == target, 1.0, 0.0)
        order = jnp.dot(
            jnp.broadcast_to(named, (8, lanes)).astype(jnp.bfloat16), upper, preferred_element_type=jnp.float32
        )[0:1, :]
        slot = lax.broadcasted_iota(jnp.int32, (cap, lanes), 0).astype(jnp.float32)
        return jnp.where(slot == order, 1.0, 0.0) * named

    def pack(s):
        q = s

        def one(ej, _):
            @pl.when(ej % 2 != core)
            def _():
                arrived(ej, q)

            select = pick(ej)[:, :rows].astype(jnp.bfloat16)
            picked = jnp.dot(select, blocks[ej, q], preferred_element_type=jnp.float32)
            packed[columns(ej * cap, cap), columns(q * width_local, width_local)] = picked.astype(jnp.bfloat16)
            return 0

        lax.fori_loop(0, n_e, one, 0)

    def relay(s):
        for o in range(1, n_x):
            arrived(lax.rem(xi + o, n_x) * 2 + core, s)
            d_copy(o, s).start()

    def forward(s):
        for o in range(1, n_x):
            x_copy(o, s).start()
        d_copy(0, s).start()

    forward(t)
    for o in range(1, n_e):
        meta_arrived(o)

    def take(side, q):
        arrived(e, q)

        @pl.when(has_next(side))
        def _():
            z_copy(side, q).start()

        forward(q)

    def finish(side, q):
        relay(q)
        pack(q)

    at_distance(1, take)
    finish(0, t)

    def dispatch(h, _):
        at_distance(h, take)
        at_distance(h - 1, finish)
        return 0

    lax.fori_loop(2, n_t, dispatch, 0)
    at_distance(n_t - 1, finish)

    def normalize(ej, _):
        at = columns(ej * cap, cap)
        weight = jnp.where(metas[ej, 0:1, :] == mine.astype(jnp.float32), metas[ej, 2:3, :], metas[ej, 3:4, :])
        wslot[at, :] = jnp.broadcast_to(jnp.sum(pick(ej) * weight, axis=1, keepdims=True), (cap, lanes))
        values = packed[at, :].astype(jnp.float32)
        scale = lax.rsqrt(jnp.sum(values * values, axis=1, keepdims=True) / width + 1e-05)
        packed[at, :] = (values * scale * gain[...]).astype(jnp.bfloat16)
        return 0

    lax.fori_loop(0, n_e, normalize, 0)

    def expert_in(j, _):
        slot = (j % pair_slots) * 2
        cols = columns(j * chunk, chunk)
        weight_copy(w_gate.at[:, cols], slot).wait()
        gate = jnp.dot(packed[...], wbuf[slot], preferred_element_type=jnp.float32)
        weight_copy(w_up.at[:, cols], slot + 1).wait()
        up = jnp.dot(packed[...], wbuf[slot + 1], preferred_element_type=jnp.float32)
        hidden[:, cols] = (gate / (1.0 + jnp.exp(-gate)) * up).astype(jnp.bfloat16)
        start_pair(j + pair_slots)
        return 0

    lax.fori_loop(0, gate_pairs, expert_in, 0)

    def o_copy(o, d):
        ej = lax.rem(e + o, n_e)
        return pltpu.make_async_remote_copy(
            src_ref=sendbuf.at[d, columns(ej * cap, cap)], dst_ref=recvbuf.at[d, columns(e * cap, cap)],
            send_sem=osend.at[o, d], recv_sem=orecv.at[e, d], device_id=(g, ej, t), device_id_type=MESH,
        )

    def o_arrived(o, d):
        ej = lax.rem(e + o, n_e)
        pltpu.make_async_remote_copy(
            src_ref=sendbuf.at[d, columns(ej * cap, cap)], dst_ref=recvbuf.at[d, columns(ej * cap, cap)],
            send_sem=osend.at[0, 0], recv_sem=orecv.at[ej, d], device_id=(g, ej, t), device_id_type=MESH,
        ).wait_recv()

    def y_copy(d):
        k, c = d // per_slice, d % per_slice
        return pltpu.make_async_remote_copy(
            src_ref=zsend.at[d], dst_ref=zrecv.at[t, c],
            send_sem=ysend.at[d], recv_sem=yrecv.at[t, c],
            device_id=(g, e, slice_of(k)), device_id_type=MESH,
        )

    def y_arrived(s, c):
        tj = lax.rem(t + s, n_t)
        pltpu.make_async_remote_copy(
            src_ref=zsend.at[0], dst_ref=zrecv.at[tj, c],
            send_sem=ysend.at[0], recv_sem=yrecv.at[tj, c],
            device_id=(g, e, tj), device_id_type=MESH,
        ).wait_recv()
        return zrecv[tj, c].astype(jnp.float32)

    def combined(d):
        for o in range(1, n_e):
            o_arrived(o, d)
        return jnp.dot(place[...], recvbuf[d], preferred_element_type=jnp.float32)

    def combine_and_send(d):
        zsend[d] = combined(d).astype(jnp.bfloat16)
        y_copy(d).start()

    def expert_out(d, _):
        slot = ((gate_pairs + d // 2) % pair_slots) * 2 + d % 2
        weight_copy(w_down.at[:, down_columns(d)], slot).wait()
        value = jnp.dot(hidden[...], wbuf[slot, 0:hid, :], preferred_element_type=jnp.float32)
        sendbuf[d] = (value * wslot[:, 0:1]).astype(jnp.bfloat16)
        for o in range(1, n_e):
            o_copy(o, d).start()
        at = columns(e * cap, cap)
        recvbuf[d, at, :] = sendbuf[d, at, :]

        @pl.when(d % 2 == 1)
        def _():
            start_pair(gate_pairs + d // 2 + pair_slots)

        @pl.when(jnp.logical_and(d >= lag, d - lag < down_chunks - per_slice))
        def _():
            combine_and_send(d - lag)

        return 0

    lax.fori_loop(0, down_chunks, expert_out, 0)

    def late(d, _):
        combine_and_send(d)
        return 0

    lax.fori_loop(max(0, down_chunks - lag), down_chunks - per_slice, late, 0)
    for c in range(per_slice):
        total = combined(down_chunks - per_slice + c)
        for s in range(1, n_t):
            total += y_arrived(s, c)
        out[:, c * chunk:(c + 1) * chunk] = total.astype(jnp.bfloat16)

    for o in range(1, n_e):
        meta_copy(o).wait_send()

    def drain_blocks(s, _):
        for side in (0, 1):
            @pl.when(jnp.logical_and(has_next(side), s <= t if side == 0 else s >= t))
            def _():
                z_copy(side, s).wait_send()

        for o in range(n_x):
            if o:
                x_copy(o, s).wait_send()
            d_copy(o, s).wait_send()
        return 0

    lax.fori_loop(0, n_t, drain_blocks, 0)

    def drain_rows(d, _):
        for o in range(1, n_e):
            o_copy(o, d).wait_send()
        return 0

    lax.fori_loop(0, down_chunks, drain_rows, 0)

    def drain_sums(d, _):
        y_copy(d).wait_send()
        return 0

    lax.fori_loop(0, down_chunks - per_slice, drain_sums, 0)


def per_device(n_e, n_t, tokens, norm_gain, w_gate, w_up, w_down, expert_ids, gate_weights):
    rows, width_local = tokens.shape
    width, hid = w_gate.shape
    cap = rows // 2
    slots = n_e * cap
    chunk = min(512, width_local, hid)
    per_slice = width_local // chunk
    down_chunks = n_t * per_slice
    pairs = hid // chunk + down_chunks // 2
    spent = 2 * (width * rows * n_e + slots * width + slots * hid + 2 * slots * width + 2 * rows * width)
    pair_slots = min(pairs, (56 * MIB - spent) // (4 * width * chunk))
    lanes = -(-rows // 128) * 128
    pad = lanes - rows
    meta = jnp.concatenate(
        [
            jnp.pad(expert_ids.T.astype(jnp.float32), ((0, 0), (0, pad)), constant_values=-1.0),
            jnp.pad(gate_weights.T, ((0, 4), (0, pad))),
        ],
        axis=0,
    )
    vmem = pl.BlockSpec(memory_space=pltpu.VMEM)
    hbm = pl.BlockSpec(memory_space=pl.ANY)
    bf16, f32, dma = jnp.bfloat16, jnp.float32, pltpu.SemaphoreType.DMA
    return pl.pallas_call(
        functools.partial(kernel, n_e, n_t, cap, chunk, pair_slots, 3),
        out_shape=jax.ShapeDtypeStruct((rows, width_local), bf16),
        in_specs=[vmem, vmem, vmem, vmem, hbm, hbm, hbm],
        out_specs=vmem,
        scratch_shapes=[
            pltpu.VMEM((2 * pair_slots, width, chunk), bf16),
            pltpu.VMEM((n_e, n_t, rows, width_local), bf16),
            pltpu.VMEM((n_e, 8, lanes), f32),
            pltpu.VMEM((slots, width), bf16),
            pltpu.VMEM((slots, hid), bf16),
            pltpu.VMEM((slots, lanes), f32),
            pltpu.VMEM((rows, slots), bf16),
            pltpu.VMEM((down_chunks, slots, chunk), bf16),
            pltpu.VMEM((down_chunks, slots, chunk), bf16),
            pltpu.VMEM((down_chunks, rows, chunk), bf16),
            pltpu.VMEM((n_t, per_slice, rows, chunk), bf16),
            dma((2 * pair_slots,)),
            dma((2,)),
            dma((n_e, n_t)),
            dma((2, n_t)),
            dma((n_e // 2, n_t)),
            dma((n_e // 2, n_t)),
            dma((n_e,)),
            dma((n_e,)),
            dma((n_e, down_chunks)),
            dma((n_e, down_chunks)),
            dma((down_chunks,)),
            dma((n_t, per_slice)),
        ],
        compiler_params=pltpu.CompilerParams(
            collective_id=0, has_side_effects=True, vmem_limit_bytes=67043328
        ),
    )(tokens, norm_gain.reshape(1, width), meta, expert_ids, w_gate, w_up, w_down)


def solution(mesh):
    in_specs = (
        P(("groups", "expert"), "tensor"),
        P(),
        P(None, ("expert", "tensor")),
        P(None, ("expert", "tensor")),
        P(("expert", "tensor"), None),
        P(("groups", "expert"), None),
        P(("groups", "expert"), None),
    )
    out_specs = P(("groups", "expert"), "tensor")
    body = functools.partial(per_device, mesh.shape["expert"], mesh.shape["tensor"])
    return jax.shard_map(body, mesh=mesh, in_specs=in_specs, out_specs=out_specs, check_vma=False)
```
